256 devices in a mesh: ep: 64 (over z, y, core), fsdp: 4 (over x).
Axes of the slice: x: 4, y: 4, z: 8, core: 2. Of those that a mesh axis runs over, the one named last changes fastest.
Arguments:
- w_down: float32 [64, 1408, 2048], P('ep', None, 'fsdp'), may hold values from -0.21875 to 0.21875
- avg_down: float32 [64, 1408, 2048], P('ep', None, 'fsdp'), may hold values from -0.15625 to 0.15625
- router_weight: float32 [2048, 64], P('fsdp', 'ep'), may hold values from -0.125 to 0.125
- router_gain: float32 [2048], P('fsdp'), may hold values from 0.25 to 1.75
Outputs:
- serve_down: bfloat16 [64, 1408, 2048], P('ep')
- scale_down: float32 [64, 1408], P('ep')
- serve_router: bfloat16 [2048, 64], replicated
- fresh_down: float32 [64, 1408, 2048], P('ep', None, 'fsdp')
The draws below stay inside these ranges and needn't reach their ends.
All inputs are finite; a program needn't handle non-finite values. Where the reference program divides by a largest or mean magnitude, that divisor is 1e-20 or more.
Results may differ from the reference program's by a relative error of at most 0.001.
Values may be sent and summed in bfloat16 or wider, within the bound.
No kernel may reach another device: no remote copies, remote signals or barrier semaphores. Data moves between devices by JAX's collectives and lax.ppermute only.
A program may use at most 64 MiB of HBM per device.

```python
import jax
import jax.numpy as jnp

EXPERTS = 64
D_MODEL = 2048
D_EXPERT = 1408


def raised(array, key, source, target, parts, factor):
    owner, partner = [(jnp.arange(array.shape[position]) // (array.shape[position] // parts)).reshape([-1 if axis == position else 1 for axis in range(array.ndim)]) for position in (source, target)]
    chosen = jax.random.permutation(key, parts)[partner]
    strong = (owner == chosen) | (owner == (partner + parts // 2) % parts)
    return jnp.where(strong, factor * array, array)


def shard_levels(stream_key, extent, split, low, largest):
    gain = 1.0
    for axis_at, parts in split:
        steps = jax.random.uniform(jax.random.fold_in(jax.random.fold_in(stream_key, 6), axis_at), (parts,), jnp.float32, low / len(split), largest / len(split))
        gain = gain * jnp.repeat(jnp.exp(steps), extent[axis_at] // parts).reshape((-1,) + (1,) * (len(extent) - 1 - axis_at))
    return gain


def normal_values(own_key, shape, scale, reach, split=(), dtype=jnp.bfloat16):
    loudness = shard_levels(own_key, shape, split, -0.22, 0.18) if split else 1.0
    drawn = jax.random.normal(own_key, shape, jnp.float32) * scale * loudness
    return jnp.minimum(jnp.maximum(drawn, -reach), reach).astype(dtype)


def heavy_noise(rng, shape, scale, limit, cuts, heavy, held_as=jnp.bfloat16):
    drawn = scale * jax.random.normal(rng, shape, jnp.float32)
    if cuts:
        drawn = drawn * shard_levels(rng, shape, cuts, -0.22, 0.18)
    return jnp.clip(raised(drawn, jax.random.fold_in(rng, 3), *heavy), -limit, limit).astype(held_as)


def setup_inputs(seed: int = 0) -> dict:
    splits = jax.random.split(jax.random.key(seed), 5)
    w_down = heavy_noise(splits[0], (EXPERTS, D_EXPERT, D_MODEL), D_EXPERT ** -0.5, 0.21875, ((0, 64), (2, 4)), (2, 1, 4, 2.0), jnp.float32)
    avg_down = normal_values(splits[1], (EXPERTS, D_EXPERT, D_MODEL), D_EXPERT ** -0.5, 0.15625, ((0, 64), (2, 4)), jnp.float32)
    router_weight = normal_values(splits[2], (D_MODEL, EXPERTS), D_MODEL ** -0.5, 0.125, ((0, 4), (1, 64)), jnp.float32)
    router_gain = jnp.clip(1.0 + 0.15 * jax.random.normal(splits[3], (D_MODEL,), jnp.float32), 0.25, 1.75)
    return {"w_down": w_down, "avg_down": avg_down, "router_weight": router_weight, "router_gain": router_gain}


def reference(w_down, avg_down, router_weight, router_gain):
    fresh_down = 0.5 * avg_down + 0.5 * w_down
    scale_down = jnp.max(jnp.abs(fresh_down), axis=2)
    serve_down = (fresh_down / jnp.expand_dims(scale_down, 2)).astype(jnp.bfloat16)
    serve_router = (router_weight * router_gain[:, None]).astype(jnp.bfloat16)
    return serve_down, scale_down, serve_router, fresh_down
```

```python
import functools

import jax
import jax.numpy as jnp
from jax import lax
from jax.experimental import pallas as pl
from jax.experimental.pallas import tpu as pltpu
from jax.sharding import PartitionSpec as P


F32, BF16 = jnp.float32, jnp.bfloat16
ANY = pl.BlockSpec(memory_space=pl.ANY)
VM = pl.BlockSpec(memory_space=pltpu.VMEM)
LANES = 128
HALF = LANES // 2
CORES, YS, ZS = 2, 4, 8
RING = (0, 1, 3, 2)
TOWER = (0, 1, 2, 3, 7, 6, 5, 4)


def in_vmem(x):
    return pltpu.with_memory_space_constraint(x, pltpu.VMEM)


def in_hbm(x):
    return pltpu.with_memory_space_constraint(x, pltpu.HBM)


def call(kernel, ins, in_specs, outs, out_specs, scratch=(), aliases=None):
    return pl.pallas_call(
        kernel,
        out_shape=outs,
        in_specs=in_specs,
        out_specs=out_specs,
        scratch_shapes=list(scratch),
        input_output_aliases=aliases or {},
        compiler_params=pltpu.CompilerParams(vmem_limit_bytes=40 * 1024 * 1024),
    )(*ins)


def run(copies):
    for copy in copies:
        copy.start()
    for copy in copies:
        copy.wait()


def fresh_kernel(groups, w_hbm, a_hbm, rw_hbm, rg_hbm, fresh_ref, msg_ref, w_buf, a_buf, r_buf, sems, r_sems):
    def copies(g):
        rows = pl.ds(g * LANES, LANES)
        return (
            pltpu.make_async_copy(w_hbm.at[0, rows, :], w_buf.at[rows, :], sems.at[0, g]),
            pltpu.make_async_copy(a_hbm.at[0, rows, :], a_buf.at[rows, :], sems.at[1, g]),
        )

    router = [
        pltpu.make_async_copy(rw_hbm, r_buf.at[0:1, :], r_sems.at[0]),
        pltpu.make_async_copy(rg_hbm, r_buf.at[1:2, :], r_sems.at[1]),
    ]
    for g in range(groups):
        for copy in copies(g):
            copy.start()
    for copy in router:
        copy.start()
    for g in range(groups):
        for copy in copies(g):
            copy.wait()
        rows = slice(g * LANES, (g + 1) * LANES)
        fresh = 0.5 * a_buf[rows, :] + 0.5 * w_buf[rows, :]
        fresh_ref[rows, :] = fresh
        size = jnp.abs(fresh)
        top = size[:, :LANES]
        for k in range(1, size.shape[1] // LANES):
            top = jnp.maximum(top, size[:, k * LANES : (k + 1) * LANES])
        msg_ref[g : g + 1, :] = jnp.max(top.T, axis=0, keepdims=True)
    for copy in router:
        copy.wait()
    part = r_buf[0:1, :] * r_buf[1:2, :]
    for k in range(part.shape[1] // LANES):
        msg_ref[groups + k : groups + k + 1, :] = part[:, k * LANES : (k + 1) * LANES]


def serve_kernel(groups, fresh_ref, m0, m1, a_ref, b_ref, scale_ref):
    scale_ref[...] = jnp.maximum(m0[:groups, :], m1[:groups, :])
    rows = a_ref.shape[0]
    for g in range(groups):
        inverse = 1.0 / scale_ref[g : g + 1, :]
        spread = jnp.broadcast_to(inverse, (LANES, LANES)).T
        for h in (0, 1):
            row = g * LANES + h * HALF
            out, at = (a_ref, row) if row < rows else (b_ref, row - rows)
            factor = spread[h * HALF : (h + 1) * HALF, :]
            for k in range(fresh_ref.shape[1] // LANES):
                lanes = slice(k * LANES, (k + 1) * LANES)
                out[at : at + HALF, lanes] = (fresh_ref[row : row + HALF, lanes] * factor).astype(BF16)


def spot(piece, out, back, row, sem):
    xs = lax.axis_size("fsdp")
    owner = lax.rem(lax.axis_index("fsdp") + (xs - back), xs)
    width = piece.shape[1]
    cols = pl.ds(pl.multiple_of(owner * width, width), width)
    return pltpu.make_async_copy(piece, out.at[0, pl.ds(row, piece.shape[0]), cols], sem)


def own_kernel(groups, a_ref, b_ref, fresh_ref, scale_ref, out, fresh_out, scale_out, line, sems):
    for g in range(groups):
        line[:, g * LANES : (g + 1) * LANES] = scale_ref[g : g + 1, :]
    run([
        spot(a_ref, out, 0, 0, sems.at[0]),
        spot(b_ref, out, 0, a_ref.shape[0], sems.at[1]),
        pltpu.make_async_copy(fresh_ref, fresh_out.at[0], sems.at[2]),
        pltpu.make_async_copy(line, scale_out, sems.at[3]),
    ])


def place_kernel(spots, *refs):
    n = len(spots)
    pieces, out, sems = refs[:n], refs[-2], refs[-1]
    run([spot(piece, out, back, row, sems.at[i]) for i, (piece, (back, row)) in enumerate(zip(pieces, spots))])


def place(out, pieces, spots):
    ins = [in_vmem(p) for p in pieces] + [out]
    return call(
        functools.partial(place_kernel, tuple(spots)),
        ins, [VM] * len(pieces) + [ANY], pltpu.HBM(out.shape, out.dtype), ANY,
        [pltpu.SemaphoreType.DMA((len(pieces),))], {len(pieces): 0},
    )


def router_rows_kernel(part, lines, out, buf):
    x, e = lax.axis_index("fsdp"), lax.axis_index("ep")
    y, c = lax.rem(e // CORES, YS), lax.rem(e, CORES)
    xs = lax.axis_size("fsdp")
    at = 0
    for yk in RING:
        for ck in range(CORES):
            row = CORES * (y ^ yk) + (c ^ ck)
            for xk in RING:
                for k in range(part):
                    buf[pl.ds((row * xs + (x ^ xk)) * part + k, 1), :] = lines[at : at + 1, :]
                    at += 1
    for j in range(xs * part):
        out[:, j * LANES : (j + 1) * LANES] = buf[pl.ds(j, CORES * YS, stride=xs * part), :].astype(BF16)


def router_place_kernel(*refs):
    pieces, out, sems = refs[:-2], refs[-2], refs[-1]
    per = CORES * YS
    z = lax.axis_index("ep") // per
    copies = []
    for piece in pieces:
        for k in range(piece.shape[0] // per):
            owner = z ^ TOWER[len(copies)]
            rows = pl.ds(pl.multiple_of(owner * per, per), per)
            copies.append(pltpu.make_async_copy(piece.at[pl.ds(k * per, per), :], out.at[rows, :], sems.at[len(copies)]))
    run(copies)


def body(w_down, avg_down, router_weight, router_gain):
    _, rows, cols = w_down.shape
    groups, half = rows // LANES, rows // 2
    xs, eps = lax.axis_size("fsdp"), lax.axis_size("ep")
    per, part = CORES * YS, cols // LANES

    def move(v, axis, to):
        return lax.ppermute(v, axis, [(i, to(i)) for i in range(lax.axis_size(axis))])

    def shift(v, by):
        return move(v, "fsdp", lambda i: (i + by) % xs)

    def swap(v, step):
        return jnp.concatenate([v, move(v, "ep", lambda e: e ^ step)], 0)

    fresh, msg = call(
        functools.partial(fresh_kernel, groups),
        (in_hbm(w_down), in_hbm(avg_down), in_hbm(router_weight.reshape(1, -1)), in_hbm(router_gain.reshape(1, -1))),
        [ANY] * 4,
        (pltpu.VMEM((rows, cols), F32), pltpu.VMEM((groups + part, LANES), F32)),
        (VM, VM),
        [
            pltpu.VMEM((rows, cols), F32), pltpu.VMEM((rows, cols), F32), pltpu.VMEM((2, cols), F32),
            pltpu.SemaphoreType.DMA((2, groups)), pltpu.SemaphoreType.DMA((2,)),
        ],
    )
    other = move(msg, "fsdp", lambda i: i ^ 1)
    msg = jnp.concatenate([jnp.maximum(msg[:groups], other[:groups]), msg[groups:], other[groups:]], 0)
    other = move(msg, "fsdp", lambda i: i ^ 3)
    a, b, scale = call(
        functools.partial(serve_kernel, groups),
        (in_vmem(fresh), in_vmem(msg), in_vmem(other)), [VM] * 3,
        (pltpu.VMEM((half, cols), BF16), pltpu.VMEM((half, cols), BF16), pltpu.VMEM((groups, LANES), F32)), (VM,) * 3,
    )
    a_r, b_l = shift(a, 1), shift(b, -1)
    b_r, a_l = shift(b, 1), shift(a, -1)
    a_rr, b_ll = shift(a_r, 1), shift(b_l, -1)

    out, fresh_out, scale_out = call(
        functools.partial(own_kernel, groups),
        [in_vmem(v) for v in (a, b, fresh, scale)], [VM] * 4,
        (pltpu.HBM((1, rows, cols * xs), BF16), pltpu.HBM((1, rows, cols), F32), pltpu.HBM((1, rows), F32)), (ANY,) * 3,
        [pltpu.VMEM((1, rows), F32), pltpu.SemaphoreType.DMA((4,))],
    )
    out = place(out, [a_r, b_l], [(1, 0), (3, half)])
    out = place(out, [b_r, a_l], [(1, half), (3, 0)])
    out = place(out, [a_rr, b_ll], [(2, 0), (2, half)])

    lines = jnp.concatenate([msg[groups:], other[groups:]], 0)
    lines = swap(lines, 1)
    lines = swap(lines, CORES)
    lines = swap(lines, CORES * 3)
    block = call(
        functools.partial(router_rows_kernel, part),
        [in_vmem(lines)], [VM],
        pltpu.VMEM((per, cols * xs), BF16), VM, [pltpu.VMEM((per * xs * part, LANES), F32)],
    )
    two = move(block, "ep", lambda e: e ^ per)
    both = jnp.concatenate([block, two], 0)
    four = move(both, "ep", lambda e: e ^ (per * 2))
    both = jnp.concatenate([both, four], 0)
    eight = move(both, "ep", lambda e: e ^ (per * 7))
    router = call(
        router_place_kernel,
        [in_vmem(both), in_vmem(eight)], [VM] * 2,
        pltpu.HBM((eps, cols * xs), BF16), ANY, [pltpu.SemaphoreType.DMA((ZS,))],
    )
    return out, scale_out, router.T, fresh_out


def solution(mesh):
    placed = (P("ep", None, "fsdp"), P("ep", None, "fsdp"), P("fsdp", "ep"), P("fsdp"))
    return jax.shard_map(
        body,
        mesh=mesh,
        in_specs=placed,
        out_specs=(P("ep", None, None), P("ep", None), P(), P("ep", None, "fsdp")),
        check_vma=False,
    )
```

```python
import functools

import jax
import jax.numpy as jnp
from jax import lax
from jax.experimental import pallas as pl
from jax.experimental.pallas import tpu as pltpu
from jax.sharding import PartitionSpec as P


F32, BF16 = jnp.float32, jnp.bfloat16
ANY = pl.BlockSpec(memory_space=pl.ANY)
VM = pl.BlockSpec(memory_space=pltpu.VMEM)
LANES = 128
HALF = LANES // 2
CORES, YS, ZS = 2, 4, 8
RING = (0, 1, 3, 2)
TOWER = (0, 1, 2, 3, 7, 6, 5, 4)


def in_vmem(x):
    return pltpu.with_memory_space_constraint(x, pltpu.VMEM)


def in_hbm(x):
    return pltpu.with_memory_space_constraint(x, pltpu.HBM)


def call(kernel, ins, in_specs, outs, out_specs, scratch=(), aliases=None):
    return pl.pallas_call(
        kernel,
        out_shape=outs,
        in_specs=in_specs,
        out_specs=out_specs,
        scratch_shapes=list(scratch),
        input_output_aliases=aliases or {},
        compiler_params=pltpu.CompilerParams(vmem_limit_bytes=12 * 1024 * 1024),
    )(*ins)


def stacked(one, two):
    low = jnp.array(-jnp.inf, one.dtype)
    return jnp.maximum(
        lax.pad(one, low, ((0, two.shape[0], 0), (0, 0, 0))),
        lax.pad(two, low, ((one.shape[0], 0, 0), (0, 0, 0))),
    )


def run(copies):
    for copy in copies:
        copy.start()
    for copy in copies:
        copy.wait()


def fresh_kernel(groups, w_hbm, a_hbm, rw_hbm, rg_hbm, fresh_ref, msg_ref, w_buf, a_buf, r_buf, sems, r_sems):
    def copies(g):
        rows = pl.ds(g * LANES, LANES)
        return (
            pltpu.make_async_copy(w_hbm.at[0, rows, :], w_buf.at[rows, :], sems.at[0, g]),
            pltpu.make_async_copy(a_hbm.at[0, rows, :], a_buf.at[rows, :], sems.at[1, g]),
        )

    router = [
        pltpu.make_async_copy(rw_hbm, r_buf.at[0:1, :], r_sems.at[0]),
        pltpu.make_async_copy(rg_hbm, r_buf.at[1:2, :], r_sems.at[1]),
    ]
    for g in range(groups):
        for copy in copies(g):
            copy.start()
    for copy in router:
        copy.start()
    for g in range(groups):
        for copy in copies(g):
            copy.wait()
        rows = slice(g * LANES, (g + 1) * LANES)
        fresh = 0.5 * a_buf[rows, :] + 0.5 * w_buf[rows, :]
        fresh_ref[rows, :] = fresh
        size = jnp.abs(fresh)
        top = size[:, :LANES]
        for k in range(1, size.shape[1] // LANES):
            top = jnp.maximum(top, size[:, k * LANES : (k + 1) * LANES])
        msg_ref[g : g + 1, :] = jnp.max(top.T, axis=0, keepdims=True)
    for copy in router:
        copy.wait()
    part = r_buf[0:1, :] * r_buf[1:2, :]
    for k in range(part.shape[1] // LANES):
        msg_ref[groups + k : groups + k + 1, :] = part[:, k * LANES : (k + 1) * LANES]


def serve_kernel(groups, fresh_ref, m0, m1, a_ref, b_ref, scale_ref):
    scale_ref[...] = jnp.maximum(m0[:groups, :], m1[:groups, :])
    rows = a_ref.shape[0]
    for g in range(groups):
        inverse = 1.0 / scale_ref[g : g + 1, :]
        spread = jnp.broadcast_to(inverse, (LANES, LANES)).T
        for h in (0, 1):
            row = g * LANES + h * HALF
            out, at = (a_ref, row) if row < rows else (b_ref, row - rows)
            factor = spread[h * HALF : (h + 1) * HALF, :]
            for k in range(fresh_ref.shape[1] // LANES):
                lanes = slice(k * LANES, (k + 1) * LANES)
                out[at : at + HALF, lanes] = (fresh_ref[row : row + HALF, lanes] * factor).astype(BF16)


def spot(piece, out, back, row, sem):
    xs = lax.axis_size("fsdp")
    owner = lax.rem(lax.axis_index("fsdp") + (xs - back), xs)
    width = piece.shape[1]
    cols = pl.ds(pl.multiple_of(owner * width, width), width)
    return pltpu.make_async_copy(piece, out.at[0, pl.ds(row, piece.shape[0]), cols], sem)


def own_kernel(groups, a_ref, b_ref, fresh_ref, scale_ref, out, fresh_out, scale_out, line, sems):
    for g in range(groups):
        line[:, g * LANES : (g + 1) * LANES] = scale_ref[g : g + 1, :]
    run([
        spot(a_ref, out, 0, 0, sems.at[0]),
        spot(b_ref, out, 0, a_ref.shape[0], sems.at[1]),
        pltpu.make_async_copy(fresh_ref, fresh_out.at[0], sems.at[2]),
        pltpu.make_async_copy(line, scale_out, sems.at[3]),
    ])


def place_kernel(spots, *refs):
    n = len(spots)
    pieces, out, sems = refs[:n], refs[-2], refs[-1]
    run([spot(piece, out, back, row, sems.at[i]) for i, (piece, (back, row)) in enumerate(zip(pieces, spots))])


def place(out, pieces, spots):
    ins = [in_vmem(p) for p in pieces] + [out]
    return call(
        functools.partial(place_kernel, tuple(spots)),
        ins, [VM] * len(pieces) + [ANY], pltpu.HBM(out.shape, out.dtype), ANY,
        [pltpu.SemaphoreType.DMA((len(pieces),))], {len(pieces): 0},
    )


def router_rows_kernel(part, lines, out, buf):
    x, e = lax.axis_index("fsdp"), lax.axis_index("ep")
    y, c = lax.rem(e // CORES, YS), lax.rem(e, CORES)
    xs = lax.axis_size("fsdp")
    at = 0
    for yk in RING:
        for ck in range(CORES):
            row = CORES * (y ^ yk) + (c ^ ck)
            for xk in RING:
                for k in range(part):
                    buf[pl.ds((row * xs + (x ^ xk)) * part + k, 1), :] = lines[at : at + 1, :]
                    at += 1
    for j in range(xs * part):
        out[:, j * LANES : (j + 1) * LANES] = buf[pl.ds(j, CORES * YS, stride=xs * part), :].astype(BF16)


def router_place_kernel(*refs):
    pieces, out, sems = refs[:-2], refs[-2], refs[-1]
    per = CORES * YS
    z = lax.axis_index("ep") // per
    copies = []
    for piece in pieces:
        for k in range(piece.shape[0] // per):
            owner = z ^ TOWER[len(copies)]
            rows = pl.ds(pl.multiple_of(owner * per, per), per)
            copies.append(pltpu.make_async_copy(piece.at[pl.ds(k * per, per), :], out.at[rows, :], sems.at[len(copies)]))
    run(copies)


def body(w_down, avg_down, router_weight, router_gain):
    _, rows, cols = w_down.shape
    groups, half = rows // LANES, rows // 2
    xs, eps = lax.axis_size("fsdp"), lax.axis_size("ep")
    per, part = CORES * YS, cols // LANES

    def move(v, axis, to):
        return lax.ppermute(v, axis, [(i, to(i)) for i in range(lax.axis_size(axis))])

    def shift(v, by):
        return move(v, "fsdp", lambda i: (i + by) % xs)

    def swap(v, step):
        return stacked(v, move(v, "ep", lambda e: e ^ step))

    fresh, msg = call(
        functools.partial(fresh_kernel, groups),
        (in_hbm(w_down), in_hbm(avg_down), in_hbm(router_weight.reshape(1, -1)), in_hbm(router_gain.reshape(1, -1))),
        [ANY] * 4,
        (pltpu.VMEM((rows, cols), F32), pltpu.VMEM((groups + part, LANES), F32)),
        (VM, VM),
        [
            pltpu.VMEM((rows, cols), F32), pltpu.VMEM((rows, cols), F32), pltpu.VMEM((2, cols), F32),
            pltpu.SemaphoreType.DMA((2, groups)), pltpu.SemaphoreType.DMA((2,)),
        ],
    )
    other = move(msg, "fsdp", lambda i: i ^ 1)
    msg = jnp.concatenate([jnp.maximum(msg[:groups], other[:groups]), msg[groups:], other[groups:]], 0)
    other = move(msg, "fsdp", lambda i: i ^ 3)
    a, b, scale = call(
        functools.partial(serve_kernel, groups),
        (in_vmem(fresh), in_vmem(msg), in_vmem(other)), [VM] * 3,
        (pltpu.VMEM((half, cols), BF16), pltpu.VMEM((half, cols), BF16), pltpu.VMEM((groups, LANES), F32)), (VM,) * 3,
    )
    a_r, b_l = shift(a, 1), shift(b, -1)
    b_r, a_l = shift(b, 1), shift(a, -1)
    a_rr, b_ll = shift(a_r, 1), shift(b_l, -1)

    out, fresh_out, scale_out = call(
        functools.partial(own_kernel, groups),
        [in_vmem(v) for v in (a, b, fresh, scale)], [VM] * 4,
        (pltpu.HBM((1, rows, cols * xs), BF16), pltpu.HBM((1, rows, cols), F32), pltpu.HBM((1, rows), F32)), (ANY,) * 3,
        [pltpu.VMEM((1, rows), F32), pltpu.SemaphoreType.DMA((4,))],
    )
    out = place(out, [a_r, b_l], [(1, 0), (3, half)])
    out = place(out, [b_r, a_l], [(1, half), (3, 0)])
    out = place(out, [a_rr, b_ll], [(2, 0), (2, half)])

    lines = stacked(msg[groups:], other[groups:])
    lines = swap(lines, 1)
    lines = swap(lines, CORES)
    lines = swap(lines, CORES * 3)
    block = call(
        functools.partial(router_rows_kernel, part),
        [in_vmem(lines)], [VM],
        pltpu.VMEM((per, cols * xs), BF16), VM, [pltpu.VMEM((per * xs * part, LANES), F32)],
    )
    two = move(block, "ep", lambda e: e ^ per)
    both = stacked(block, two)
    four = move(both, "ep", lambda e: e ^ (per * 2))
    both = stacked(both, four)
    eight = move(both, "ep", lambda e: e ^ (per * 7))
    router = call(
        router_place_kernel,
        [in_vmem(both), in_vmem(eight)], [VM] * 2,
        pltpu.HBM((eps, cols * xs), BF16), ANY, [pltpu.SemaphoreType.DMA((ZS,))],
    )
    return out, scale_out, router.T, fresh_out


def solution(mesh):
    placed = (P("ep", None, "fsdp"), P("ep", None, "fsdp"), P("fsdp", "ep"), P("fsdp"))
    return jax.shard_map(
        body,
        mesh=mesh,
        in_specs=placed,
        out_specs=(P("ep", None, None), P("ep", None), P(), P("ep", None, "fsdp")),
        check_vma=False,
    )
```

```python
import functools

import jax
import jax.numpy as jnp
from jax import lax
from jax.experimental import pallas as pl
from jax.experimental.pallas import tpu as pltpu
from jax.sharding import PartitionSpec as P


F32, BF16 = jnp.float32, jnp.bfloat16
ANY = pl.BlockSpec(memory_space=pl.ANY)
VM = pl.BlockSpec(memory_space=pltpu.VMEM)
LANES = 128
HALF = LANES // 2
CORES, YS, ZS = 2, 4, 8
RING = (0, 1, 3, 2)
TOWER = (0, 1, 2, 3, 7, 6, 5, 4)


def in_vmem(x):
    return pltpu.with_memory_space_constraint(x, pltpu.VMEM)


def in_hbm(x):
    return pltpu.with_memory_space_constraint(x, pltpu.HBM)


def call(kernel, ins, in_specs, outs, out_specs, scratch=(), aliases=None):
    return pl.pallas_call(
        kernel,
        out_shape=outs,
        in_specs=in_specs,
        out_specs=out_specs,
        scratch_shapes=list(scratch),
        input_output_aliases=aliases or {},
        compiler_params=pltpu.CompilerParams(vmem_limit_bytes=12 * 1024 * 1024),
    )(*ins)


def stacked(one, two):
    low = jnp.array(-jnp.inf, one.dtype)
    return jnp.maximum(
        lax.pad(one, low, ((0, two.shape[0], 0), (0, 0, 0))),
        lax.pad(two, low, ((one.shape[0], 0, 0), (0, 0, 0))),
    )


def run(copies):
    for copy in copies:
        copy.start()
    for copy in copies:
        copy.wait()


def fresh_kernel(groups, w_hbm, a_hbm, rw_hbm, rg_hbm, fresh_ref, early_ref, msg_ref, w_buf, a_buf, r_buf, sems, r_sems):
    def copies(g):
        rows = pl.ds(g * LANES, LANES)
        return (
            pltpu.make_async_copy(w_hbm.at[0, rows, :], w_buf.at[rows, :], sems.at[0, g]),
            pltpu.make_async_copy(a_hbm.at[0, rows, :], a_buf.at[rows, :], sems.at[1, g]),
        )

    router = [
        pltpu.make_async_copy(rw_hbm, r_buf.at[0:1, :], r_sems.at[0]),
        pltpu.make_async_copy(rg_hbm, r_buf.at[1:2, :], r_sems.at[1]),
    ]
    for g in range(groups):
        for copy in copies(g):
            copy.start()
    for copy in router:
        copy.start()
    for g in range(groups):
        for copy in copies(g):
            copy.wait()
        rows = slice(g * LANES, (g + 1) * LANES)
        fresh = 0.5 * a_buf[rows, :] + 0.5 * w_buf[rows, :]
        fresh_ref[rows, :] = fresh
        if (g + 1) * LANES <= early_ref.shape[0]:
            early_ref[rows, :] = fresh
        size = jnp.abs(fresh)
        top = size[:, :LANES]
        for k in range(1, size.shape[1] // LANES):
            top = jnp.maximum(top, size[:, k * LANES : (k + 1) * LANES])
        msg_ref[g : g + 1, :] = jnp.max(top.T, axis=0, keepdims=True)
    for copy in router:
        copy.wait()
    part = r_buf[0:1, :] * r_buf[1:2, :]
    for k in range(part.shape[1] // LANES):
        msg_ref[groups + k : groups + k + 1, :] = part[:, k * LANES : (k + 1) * LANES]


def scaled(scale, g):
    return jnp.broadcast_to(1.0 / scale[g : g + 1, :], (LANES, LANES)).T


def serve_kernel(groups, fresh_ref, m0, m1, m2, m3, e_ref, a_ref, b_ref, scale_ref):
    scale_ref[...] = jnp.maximum(
        jnp.maximum(m0[:groups, :], m1[:groups, :]), jnp.maximum(m2[:groups, :], m3[:groups, :])
    )
    spots, row = {}, 0
    for out in (e_ref, a_ref, b_ref):
        for at in range(0, out.shape[0], HALF):
            spots[row + at] = (out, at)
        row += out.shape[0]
    for g in range(groups):
        spread = scaled(scale_ref, g)
        for h in (0, 1):
            row = g * LANES + h * HALF
            out, at = spots[row]
            factor = spread[h * HALF : (h + 1) * HALF, :]
            for k in range(fresh_ref.shape[1] // LANES):
                lanes = slice(k * LANES, (k + 1) * LANES)
                out[at : at + HALF, lanes] = (fresh_ref[row : row + HALF, lanes] * factor).astype(BF16)


def early_kernel(r_ref, l_ref, scale_ref, r_out, l_out):
    for g in range(r_ref.shape[0] // LANES):
        spread = scaled(scale_ref, g)
        rows = slice(g * LANES, (g + 1) * LANES)
        for ref, out in ((r_ref, r_out), (l_ref, l_out)):
            for k in range(ref.shape[1] // LANES):
                lanes = slice(k * LANES, (k + 1) * LANES)
                out[rows, lanes] = (ref[rows, lanes] * spread).astype(BF16)


def spot(piece, out, back, row, sem):
    xs = lax.axis_size("fsdp")
    owner = lax.rem(lax.axis_index("fsdp") + (xs - back), xs)
    width = piece.shape[1]
    cols = pl.ds(pl.multiple_of(owner * width, width), width)
    return pltpu.make_async_copy(piece, out.at[0, pl.ds(row, piece.shape[0]), cols], sem)


def own_kernel(groups, e_ref, a_ref, b_ref, fresh_ref, scale_ref, out, fresh_out, scale_out, line, sems):
    for g in range(groups):
        line[:, g * LANES : (g + 1) * LANES] = scale_ref[g : g + 1, :]
    copies, row = [], 0
    for piece in (e_ref, a_ref, b_ref):
        copies.append(spot(piece, out, 0, row, sems.at[len(copies)]))
        row += piece.shape[0]
    copies.append(pltpu.make_async_copy(fresh_ref, fresh_out.at[0], sems.at[3]))
    copies.append(pltpu.make_async_copy(line, scale_out, sems.at[4]))
    run(copies)


def place_kernel(spots, *refs):
    n = len(spots)
    pieces, out, sems = refs[:n], refs[-2], refs[-1]
    run([spot(piece, out, back, row, sems.at[i]) for i, (piece, (back, row)) in enumerate(zip(pieces, spots))])


def place(out, pieces, spots):
    ins = [in_vmem(p) for p in pieces] + [out]
    return call(
        functools.partial(place_kernel, tuple(spots)),
        ins, [VM] * len(pieces) + [ANY], pltpu.HBM(out.shape, out.dtype), ANY,
        [pltpu.SemaphoreType.DMA((len(pieces),))], {len(pieces): 0},
    )


def router_rows_kernel(part, lines, out, buf):
    x, e = lax.axis_index("fsdp"), lax.axis_index("ep")
    y, c = lax.rem(e // CORES, YS), lax.rem(e, CORES)
    xs = lax.axis_size("fsdp")
    at = 0
    for yk in RING:
        for ck in range(CORES):
            row = CORES * (y ^ yk) + (c ^ ck)
            for back in range(xs):
                col = lax.rem(x + (xs - back), xs)
                for k in range(part):
                    buf[pl.ds((row * xs + col) * part + k, 1), :] = lines[at : at + 1, :]
                    at += 1
    for j in range(xs * part):
        out[:, j * LANES : (j + 1) * LANES] = buf[pl.ds(j, CORES * YS, stride=xs * part), :].astype(BF16)


def router_place_kernel(*refs):
    pieces, out, sems = refs[:-2], refs[-2], refs[-1]
    per = CORES * YS
    z = lax.axis_index("ep") // per
    copies = []
    for piece in pieces:
        for k in range(piece.shape[0] // per):
            owner = z ^ TOWER[len(copies)]
            rows = pl.ds(pl.multiple_of(owner * per, per), per)
            copies.append(pltpu.make_async_copy(piece.at[pl.ds(k * per, per), :], out.at[rows, :], sems.at[len(copies)]))
    run(copies)


def body(w_down, avg_down, router_weight, router_gain):
    _, rows, cols = w_down.shape
    groups = rows // LANES
    ne = LANES
    na = (rows - 2 * ne) // 2
    nb = rows - ne - na
    xs, eps = lax.axis_size("fsdp"), lax.axis_size("ep")
    per, part = CORES * YS, cols // LANES

    def move(v, axis, to):
        return lax.ppermute(v, axis, [(i, to(i)) for i in range(lax.axis_size(axis))])

    def shift(v, by):
        return move(v, "fsdp", lambda i: (i + by) % xs)

    def swap(v, step):
        return stacked(v, move(v, "ep", lambda e: e ^ step))

    fresh, early, msg = call(
        functools.partial(fresh_kernel, groups),
        (in_hbm(w_down), in_hbm(avg_down), in_hbm(router_weight.reshape(1, -1)), in_hbm(router_gain.reshape(1, -1))),
        [ANY] * 4,
        (pltpu.VMEM((rows, cols), F32), pltpu.VMEM((ne, cols), F32), pltpu.VMEM((groups + part, LANES), F32)),
        (VM,) * 3,
        [
            pltpu.VMEM((rows, cols), F32), pltpu.VMEM((rows, cols), F32), pltpu.VMEM((2, cols), F32),
            pltpu.SemaphoreType.DMA((2, groups)), pltpu.SemaphoreType.DMA((2,)),
        ],
    )
    m2, m1, m3 = shift(msg, 2), shift(msg, 1), shift(msg, -1)
    e_r, e_l = shift(early, 1), shift(early, -1)
    e, a, b, scale = call(
        functools.partial(serve_kernel, groups),
        [in_vmem(v) for v in (fresh, msg, m1, m2, m3)], [VM] * 5,
        (*(pltpu.VMEM((n, cols), BF16) for n in (ne, na, nb)), pltpu.VMEM((groups, LANES), F32)), (VM,) * 4,
    )
    a_r, b_l = shift(a, 1), shift(b, -1)
    b_r, a_l = shift(b, 1), shift(a, -1)
    e_r, e_l = call(
        early_kernel,
        [in_vmem(v) for v in (e_r, e_l, scale)], [VM] * 3,
        (pltpu.VMEM((ne, cols), BF16),) * 2, (VM,) * 2,
    )
    e_rr = shift(e_r, 1)
    a_rr, b_ll = shift(a_r, 1), shift(b_l, -1)

    out, fresh_out, scale_out = call(
        functools.partial(own_kernel, groups),
        [in_vmem(v) for v in (e, a, b, fresh, scale)], [VM] * 5,
        (pltpu.HBM((1, rows, cols * xs), BF16), pltpu.HBM((1, rows, cols), F32), pltpu.HBM((1, rows), F32)), (ANY,) * 3,
        [pltpu.VMEM((1, rows), F32), pltpu.SemaphoreType.DMA((5,))],
    )
    at_a, at_b = ne, ne + na
    out = place(out, [e_r, e_l, a_r, b_l], [(1, 0), (3, 0), (1, at_a), (3, at_b)])
    out = place(out, [b_r, a_l, e_rr], [(1, at_b), (3, at_a), (2, 0)])
    out = place(out, [a_rr, b_ll], [(2, at_a), (2, at_b)])

    lines = stacked(stacked(msg[groups:], m1[groups:]), stacked(m2[groups:], m3[groups:]))
    lines = swap(lines, 1)
    lines = swap(lines, CORES)
    lines = swap(lines, CORES * 3)
    block = call(
        functools.partial(router_rows_kernel, part),
        [in_vmem(lines)], [VM],
        pltpu.VMEM((per, cols * xs), BF16), VM, [pltpu.VMEM((per * xs * part, LANES), F32)],
    )
    two = move(block, "ep", lambda e: e ^ per)
    both = stacked(block, two)
    four = move(both, "ep", lambda e: e ^ (per * 2))
    both = stacked(both, four)
    eight = move(both, "ep", lambda e: e ^ (per * 7))
    router = call(
        router_place_kernel,
        [in_vmem(both), in_vmem(eight)], [VM] * 2,
        pltpu.HBM((eps, cols * xs), BF16), ANY, [pltpu.SemaphoreType.DMA((ZS,))],
    )
    return out, scale_out, router.T, fresh_out


def solution(mesh):
    placed = (P("ep", None, "fsdp"), P("ep", None, "fsdp"), P("fsdp", "ep"), P("fsdp"))
    return jax.shard_map(
        body,
        mesh=mesh,
        in_specs=placed,
        out_specs=(P("ep", None, None), P("ep", None), P(), P("ep", None, "fsdp")),
        check_vma=False,
    )
```

```python
import functools

import jax
import jax.numpy as jnp
from jax import lax
from jax.experimental import pallas as pl
from jax.experimental.pallas import tpu as pltpu
from jax.sharding import PartitionSpec as P


F32, BF16 = jnp.float32, jnp.bfloat16
ANY = pl.BlockSpec(memory_space=pl.ANY)
VM = pl.BlockSpec(memory_space=pltpu.VMEM)
LANES = 128
HALF = LANES // 2
CORES, YS, ZS = 2, 4, 8
RING = (0, 1, 3, 2)
TOWER = (0, 1, 2, 3, 7, 6, 5, 4)
STEPS, MIDDLE = 248.0, 124.0
TINY = 1e-30


def in_vmem(x):
    return pltpu.with_memory_space_constraint(x, pltpu.VMEM)


def in_hbm(x):
    return pltpu.with_memory_space_constraint(x, pltpu.HBM)


def call(kernel, ins, in_specs, outs, out_specs, scratch=(), aliases=None):
    return pl.pallas_call(
        kernel,
        out_shape=outs,
        in_specs=in_specs,
        out_specs=out_specs,
        scratch_shapes=list(scratch),
        input_output_aliases=aliases or {},
        compiler_params=pltpu.CompilerParams(vmem_limit_bytes=12 * 1024 * 1024),
    )(*ins)


def stacked(one, two):
    low = jnp.array(-jnp.inf, one.dtype)
    return jnp.maximum(
        lax.pad(one, low, ((0, two.shape[0], 0), (0, 0, 0))),
        lax.pad(two, low, ((one.shape[0], 0, 0), (0, 0, 0))),
    )


def run(copies):
    for copy in copies:
        copy.start()
    for copy in copies:
        copy.wait()


def spread(line):
    return jnp.broadcast_to(line, (LANES, LANES)).T


def lanes_of(width):
    return [slice(k * LANES, (k + 1) * LANES) for k in range(width // LANES)]


def fresh_kernel(start, groups, chunks, router, w_hbm, a_hbm, *refs):
    refs = list(refs)
    r_hbm = [refs.pop(0) for _ in range(2 * router)]
    fresh_ref, top_ref = refs.pop(0), refs.pop(0)
    outs = [refs.pop(0) for _ in chunks]
    w_buf, a_buf, r_buf, sems, r_sems = refs

    def copies(g):
        there, here = pl.ds(start + g * LANES, LANES), pl.ds(g * LANES, LANES)
        return (
            pltpu.make_async_copy(w_hbm.at[0, there, :], w_buf.at[here, :], sems.at[0, g]),
            pltpu.make_async_copy(a_hbm.at[0, there, :], a_buf.at[here, :], sems.at[1, g]),
        )

    part = [pltpu.make_async_copy(ref, r_buf.at[k : k + 1, :], r_sems.at[k]) for k, ref in enumerate(r_hbm)]
    for g in range(groups):
        for copy in copies(g):
            copy.start()
    for copy in part:
        copy.start()
    blocks = lanes_of(fresh_ref.shape[1])
    for g in range(groups):
        for copy in copies(g):
            copy.wait()
        rows = slice(g * LANES, (g + 1) * LANES)
        top = None
        for lanes in blocks:
            fresh = 0.5 * a_buf[rows, lanes] + 0.5 * w_buf[rows, lanes]
            fresh_ref[rows, lanes] = fresh
            size = jnp.abs(fresh)
            top = size if top is None else jnp.maximum(top, size)
        line = jnp.max(top.T, axis=0, keepdims=True)
        top_ref[g : g + 1, :] = line
        inverse = spread(STEPS / jnp.maximum(line, TINY))
        for h in (0, 1):
            row = g * LANES + h * HALF
            factor = inverse[h * HALF : (h + 1) * HALF, :]
            for lanes in blocks:
                x = fresh_ref[row : row + HALF, lanes]
                code = jnp.exp2(jnp.abs(x) * factor - MIDDLE)
                code = jnp.where(x < 0, -code, code).astype(BF16)
                for out, (first, end) in zip(outs, chunks):
                    if first <= row < end:
                        out[row - first : row - first + HALF, lanes] = code
    if router:
        for copy in part:
            copy.wait()
        product = r_buf[0:1, :] * r_buf[1:2, :]
        for k, lanes in enumerate(blocks):
            top_ref[groups + k : groups + k + 1, :] = product[:, lanes]


def largest(msgs, g):
    out = msgs[0][g : g + 1, :]
    for msg in msgs[1:]:
        out = jnp.maximum(out, msg[g : g + 1, :])
    return out


def spot(piece, out, back, row, sem):
    xs = lax.axis_size("fsdp")
    owner = lax.rem(lax.axis_index("fsdp") + (xs - back), xs)
    width = piece.shape[1]
    cols = pl.ds(pl.multiple_of(owner * width, width), width)
    return pltpu.make_async_copy(piece, out.at[0, pl.ds(row, piece.shape[0]), cols], sem)


def own_kernel(groups, first, m0, m1, m2, m3, f_ref, g_ref, out, fresh_out, scale_out, line, buf, sems):
    upper, lower = pl.ds(0, first), pl.ds(first, g_ref.shape[0])
    copies = [
        pltpu.make_async_copy(f_ref, fresh_out.at[0, upper, :], sems.at[0]),
        pltpu.make_async_copy(g_ref, fresh_out.at[0, lower, :], sems.at[1]),
    ]
    for copy in copies:
        copy.start()
    for g in range(groups):
        scale = largest((m0, m1, m2, m3), g)
        line[:, g * LANES : (g + 1) * LANES] = scale
        inverse = spread(1.0 / scale)
        ref, at = (f_ref, g * LANES) if g * LANES < first else (g_ref, g * LANES - first)
        for lanes in lanes_of(buf.shape[1]):
            buf[g * LANES : (g + 1) * LANES, lanes] = (ref[at : at + LANES, lanes] * inverse).astype(BF16)
    late = [spot(buf, out, 0, 0, sems.at[2]), pltpu.make_async_copy(line, scale_out, sems.at[3])]
    for copy in late:
        copy.start()
    for copy in copies + late:
        copy.wait()


def land_kernel(spots, m0, m1, m2, m3, *refs):
    n = len(spots)
    msgs = (m0, m1, m2, m3)
    pieces, out, bufs, sems = refs[:n], refs[-n - 2], refs[-n - 1 : -1], refs[-1]
    copies = []
    for i, (piece, buf, (back, row)) in enumerate(zip(pieces, bufs, spots)):
        factors = {}
        for at in range(0, piece.shape[0], HALF):
            g, h = divmod(row + at, LANES)
            if g not in factors:
                own = jnp.maximum(msgs[back][g : g + 1, :], TINY)
                factors[g] = spread(own / (STEPS * largest(msgs, g)))
            factor = factors[g][h : h + HALF, :]
            for lanes in lanes_of(piece.shape[1]):
                code = piece[at : at + HALF, lanes].astype(F32)
                size = (jnp.log2(jnp.abs(code)) + MIDDLE) * factor
                buf[at : at + HALF, lanes] = jnp.where(code < 0, -size, size).astype(BF16)
        copies.append(spot(buf, out, back, row, sems.at[i]))
        copies[-1].start()
    for copy in copies:
        copy.wait()


def land(out, msgs, pieces, spots):
    ins = [in_vmem(p) for p in (*msgs, *pieces)] + [out]
    n = len(pieces)
    return call(
        functools.partial(land_kernel, tuple(spots)),
        ins, [VM] * (4 + n) + [ANY], pltpu.HBM(out.shape, out.dtype), ANY,
        [*(pltpu.VMEM(p.shape, BF16) for p in pieces), pltpu.SemaphoreType.DMA((n,))], {4 + n: 0},
    )


def router_rows_kernel(part, lines, out, buf):
    x, e = lax.axis_index("fsdp"), lax.axis_index("ep")
    y, c = lax.rem(e // CORES, YS), lax.rem(e, CORES)
    xs = lax.axis_size("fsdp")
    at = 0
    for yk in RING:
        for ck in range(CORES):
            row = CORES * (y ^ yk) + (c ^ ck)
            for back in range(xs):
                col = lax.rem(x + (xs - back), xs)
                for k in range(part):
                    buf[pl.ds((row * xs + col) * part + k, 1), :] = lines[at : at + 1, :]
                    at += 1
    for j in range(xs * part):
        out[:, j * LANES : (j + 1) * LANES] = buf[pl.ds(j, CORES * YS, stride=xs * part), :].astype(BF16)


def router_place_kernel(*refs):
    pieces, out, sems = refs[:-2], refs[-2], refs[-1]
    per = CORES * YS
    z = lax.axis_index("ep") // per
    copies = []
    for piece in pieces:
        for k in range(piece.shape[0] // per):
            owner = z ^ TOWER[len(copies)]
            rows = pl.ds(pl.multiple_of(owner * per, per), per)
            copies.append(pltpu.make_async_copy(piece.at[pl.ds(k * per, per), :], out.at[rows, :], sems.at[len(copies)]))
    run(copies)


def body(w_down, avg_down, router_weight, router_gain):
    _, rows, cols = w_down.shape
    groups = rows // LANES
    nc, na = 4 * LANES, LANES + HALF
    nb = nc
    at_a, at_b, at_d = nc, nc + na, nc + na + nb
    xs, eps = lax.axis_size("fsdp"), lax.axis_size("ep")
    per, part = CORES * YS, cols // LANES

    def move(v, axis, to):
        return lax.ppermute(v, axis, [(i, to(i)) for i in range(lax.axis_size(axis))])

    def shift(v, by):
        return move(v, "fsdp", lambda i: (i + by) % xs)

    def swap(v, step):
        return stacked(v, move(v, "ep", lambda e: e ^ step))

    def front(start, count, chunks, router):
        refs = [in_hbm(w_down), in_hbm(avg_down)]
        if router:
            refs += [in_hbm(router_weight.reshape(1, -1)), in_hbm(router_gain.reshape(1, -1))]
        return call(
            functools.partial(fresh_kernel, start, count, chunks, router),
            refs, [ANY] * len(refs),
            (
                pltpu.VMEM((count * LANES, cols), F32), pltpu.VMEM((count + part * router, LANES), F32),
                *(pltpu.VMEM((end - first, cols), BF16) for first, end in chunks),
            ),
            (VM,) * (2 + len(chunks)),
            [
                pltpu.VMEM((count * LANES, cols), F32), pltpu.VMEM((count * LANES, cols), F32), pltpu.VMEM((2, cols), F32),
                pltpu.SemaphoreType.DMA((2, count)), pltpu.SemaphoreType.DMA((2,)),
            ],
        )

    first = nc // LANES
    fresh_c, top_c, c = front(0, first, ((0, nc),), False)
    c_r, c_l = shift(c, 1), shift(c, -1)
    fresh_r, top_r, a, bd = front(nc, groups - first, ((0, na), (na, rows - nc)), True)
    msg = stacked(top_c, top_r)
    m2, m1, m3 = shift(msg, 2), shift(msg, 1), shift(msg, -1)
    msgs = [msg, m1, m2, m3]
    a_r, bd_l = shift(a, 1), shift(bd, -1)
    bd_r, a_l = shift(bd, 1), shift(a, -1)
    c_rr, a_rr = shift(c_r, 1), shift(a_r, 1)
    b_ll, d_ll = shift(bd_l[:nb], -1), shift(bd_l[nb:], -1)

    out, fresh_out, scale_out = call(
        functools.partial(own_kernel, groups, nc),
        [in_vmem(v) for v in (*msgs, fresh_c, fresh_r)], [VM] * 6,
        (pltpu.HBM((1, rows, cols * xs), BF16), pltpu.HBM((1, rows, cols), F32), pltpu.HBM((1, rows), F32)), (ANY,) * 3,
        [pltpu.VMEM((1, rows), F32), pltpu.VMEM((rows, cols), BF16), pltpu.SemaphoreType.DMA((4,))],
    )
    out = land(out, msgs, [c_r, c_l], [(1, 0), (3, 0)])
    out = land(out, msgs, [a_r, bd_l], [(1, at_a), (3, at_b)])
    out = land(out, msgs, [bd_r, a_l], [(1, at_b), (3, at_a)])
    out = land(out, msgs, [c_rr, b_ll], [(2, 0), (2, at_b)])
    out = land(out, msgs, [a_rr, d_ll], [(2, at_a), (2, at_d)])

    lines = stacked(stacked(msg[groups:], m1[groups:]), stacked(m2[groups:], m3[groups:]))
    lines = swap(lines, 1)
    lines = swap(lines, CORES)
    lines = swap(lines, CORES * 3)
    block = call(
        functools.partial(router_rows_kernel, part),
        [in_vmem(lines)], [VM],
        pltpu.VMEM((per, cols * xs), BF16), VM, [pltpu.VMEM((per * xs * part, LANES), F32)],
    )
    two = move(block, "ep", lambda e: e ^ per)
    both = stacked(block, two)
    four = move(both, "ep", lambda e: e ^ (per * 2))
    both = stacked(both, four)
    eight = move(both, "ep", lambda e: e ^ (per * 7))
    router = call(
        router_place_kernel,
        [in_vmem(both), in_vmem(eight)], [VM] * 2,
        pltpu.HBM((eps, cols * xs), BF16), ANY, [pltpu.SemaphoreType.DMA((ZS,))],
    )
    return out, scale_out, router.T, fresh_out


def solution(mesh):
    placed = (P("ep", None, "fsdp"), P("ep", None, "fsdp"), P("fsdp", "ep"), P("fsdp"))
    return jax.shard_map(
        body,
        mesh=mesh,
        in_specs=placed,
        out_specs=(P("ep", None, None), P("ep", None), P(), P("ep", None, "fsdp")),
        check_vma=False,
    )
```
